256 devices in a mesh: batch: 16 (over z, core), vocab: 16 (over y, x).
Axes of the slice: x: 4, y: 4, z: 8, core: 2. Of those that a mesh axis runs over, the one named last changes fastest.
Arguments:
- hidden: bfloat16 [2048, 4096], P('batch'), may hold values from -40 to 40
- exit_layer: int32 [2048], P('batch'), may hold values from 0 to 7
- exit_gains: float32 [8, 4096], replicated, may hold values from 0.1 to 1.9
- unembed: bfloat16 [4096, 128256], P(None, ('batch', 'vocab')), may hold values from -10 to 10
- targets: int32 [2048], replicated, may hold values from 0 to 128255
- values: float32 [2048], P('batch'), may hold values from -6 to 6
- rewards: float32 [2048], P('batch'), may hold values from -2 to 2
- ref_logprob: float32 [2048], P('batch'), may hold values from -16 to -6
- segment_end: int32 [2048], P('batch'), may hold values 0 or 1
Outputs:
- logprob: float32 [2048], P('batch')
- advantages: float32 [2048], P('batch')
The draws below stay inside these ranges and needn't reach their ends.
All inputs are finite; a program needn't handle non-finite values. No bound on the sum of `segment_end` on one device may be relied on, other than what follows from the above.
Results may differ from the reference program's by a relative error of at most 0.00054.
Values may be sent and summed in bfloat16 or wider, within the bound.
A program may use at most 128 MiB of HBM per device.

```python
import math
import jax
import jax.numpy as jnp
import numpy as np
from jax import lax

D = 4096
VOCAB = 128256
EXITS = 8
TOK_B = 128
TOKENS = 2048


def draw_hidden(key, part):
    keys = jax.random.split(jax.random.fold_in(key, 1), 3)
    base = jnp.clip(jax.random.normal(keys[0], (TOKENS, D), jnp.float32), -4.0, 4.0)
    row_scale = jnp.exp(jax.random.uniform(keys[1], (TOKENS, 1), jnp.float32) * jnp.log(10.0))
    col_scale = jnp.exp(jax.random.uniform(keys[2], (1, D), jnp.float32) * jnp.log(10.0))
    result = base * row_scale * col_scale / 10.0
    return result.astype(jnp.bfloat16)


def draw_unembed(key, part):
    base = jnp.clip(jax.random.normal(jax.random.fold_in(key, 2), (D, VOCAB), jnp.float32), -4.0, 4.0)
    result = base * (3.0 / jnp.sqrt(jnp.float32(D)))
    return result.astype(jnp.bfloat16)


def with_ends(values, stream_key, smallest, top_value):
    shape = values.shape
    place = [jax.random.randint(jax.random.fold_in(stream_key, axis), (), 0, shape[axis]) for axis in range(len(shape))]
    values = values.at[tuple(place)].set(smallest)
    longest = shape.index(max(shape))
    place[longest] = (place[longest] + 1) % shape[longest]
    return values.at[tuple(place)].set(top_value)


def shard_levels(stream_key, extent, pieces, least, high):
    gain, own = 1.0, jax.random.fold_in(stream_key, 6)
    for position, blocks in pieces:
        steps = jnp.exp(jax.random.uniform(jax.random.fold_in(own, position), (blocks,), jnp.float32, least / len(pieces), high / len(pieces)))
        gain = gain * jnp.repeat(steps, extent[position] // blocks).reshape([-1 if axis == position else 1 for axis in range(len(extent))])
    return gain


def ranked_wide(stream_key, extent, count, lean):
    portions = [min(1 << octave, count + 1 - (1 << octave)) * (1 << 20) // math.isqrt((1 << octave) ** lean) + 1 for octave in range((count + 1).bit_length()) if 1 << octave <= count]
    spread = 1 + sum(portions) // (1 << 30)
    table = np.cumsum(np.array([max(1, weight // spread) for weight in portions]))
    pick = jax.random.randint(jax.random.fold_in(stream_key, 1), extent, 0, int(table[len(portions) - 1]))
    start = jnp.left_shift(1, jnp.searchsorted(jnp.asarray(table, jnp.int32), pick, side="right").astype(jnp.int32))
    grade = start - 1 + jax.random.randint(jax.random.fold_in(stream_key, 4), extent, 0, 1 << 30) % jnp.minimum(start, count + 1 - start)
    return jax.random.permutation(jax.random.fold_in(stream_key, 2), count)[grade].astype(jnp.int32)


def gaussian(own_key, shape, deviation, reach, pieces=(), held_as=jnp.bfloat16):
    drawn = deviation * jax.random.normal(own_key, shape, jnp.float32)
    if pieces:
        drawn = drawn * shard_levels(own_key, shape, pieces, -0.22, 0.18)
    return jnp.clip(drawn, -reach, reach).astype(held_as)


def setup_inputs(seed: int = 0) -> dict:
    splits = jax.random.split(jax.random.key(seed), 10)
    return {
        "hidden": draw_hidden(jax.random.fold_in(splits[9], 71), 0),
        "exit_layer": with_ends(jax.random.randint(splits[1], (TOKENS,), 0, EXITS), jax.random.fold_in(splits[1], 1), 0, EXITS - 1).astype(jnp.int32),
        "exit_gains": jnp.clip(1.0 + 0.18 * jax.random.normal(splits[2], (EXITS, D), jnp.float32), 0.1, 1.9),
        "unembed": draw_unembed(jax.random.fold_in(splits[9], 71), 0),
        "targets": with_ends(ranked_wide(splits[4], (TOKENS,), VOCAB, 2), jax.random.fold_in(splits[4], 3), 0, VOCAB - 1).astype(jnp.int32),
        "values": gaussian(splits[5], (TOKENS,), 1.0, 6.0, ((0, 16),), jnp.float32),
        "rewards": gaussian(splits[6], (TOKENS,), 0.3, 2.0, ((0, 16),), jnp.float32),
        "ref_logprob": jnp.clip(-16.0 + 10.0 * jax.random.uniform(splits[7], (TOKENS,), jnp.float32) ** shard_levels(splits[7], (TOKENS,), ((0, 16),), -0.2, 0.2), -16.0, -6.0),
        "segment_end": with_ends((jax.random.randint(splits[8], (TOKENS,), 0, 4 * TOK_B) < 1).astype(jnp.int32), jax.random.fold_in(splits[8], 1), 0, 1),
    }


epsilon_norm = 1e-05
discount = 1.0
trace_decay = 0.999
penalty_weight = 0.1

def reference(hidden, exit_layer, exit_gains, unembed, targets, values, rewards, ref_logprob, segment_end):
    states = hidden.astype(jnp.float32)
    inverse = lax.rsqrt(lax.optimization_barrier(jnp.mean(states * states, axis=-1, keepdims=True)) + epsilon_norm)
    normed = (states * inverse * exit_gains[exit_layer]).astype(jnp.bfloat16)
    weight_wide = unembed.astype(jnp.float32)

    def score_block(pair):
        block_rows, block_ids = pair
        logits = jnp.dot(block_rows.astype(jnp.float32), weight_wide, precision=lax.Precision.HIGHEST)
        row_max = lax.optimization_barrier(jnp.max(logits, axis=1))
        row_total = lax.optimization_barrier(jnp.sum(jnp.exp(logits - row_max[:, None]), axis=1))
        picked = jnp.take_along_axis(logits, block_ids[:, None], axis=1)[:, 0]
        return picked - (row_max + jnp.log(row_total))
    blocks = TOKENS // TOK_B
    logprob = lax.map(score_block, (normed.reshape(blocks, TOK_B, D), targets.reshape(blocks, TOK_B))).reshape(TOKENS)
    keeping = 1.0 - segment_end.astype(jnp.float32)
    next_values = jnp.concatenate([values[1:], jnp.zeros((1,), jnp.float32)])
    shaped = rewards - penalty_weight * (logprob - ref_logprob)
    deltas = shaped + discount * next_values * keeping - values
    factors = discount * trace_decay * keeping

    def backward(running, inputs):
        factor, delta = inputs
        running = delta + factor * running
        return (running, running)
    finished, advantages = lax.scan(backward, jnp.zeros((), jnp.float32), (factors, deltas), reverse=True)
    return (logprob, advantages)
```

```python
import functools

import jax
import jax.numpy as jnp
from jax import lax
from jax.experimental import pallas as pl
from jax.experimental.pallas import tpu as pltpu
from jax.sharding import Mesh
from jax.sharding import PartitionSpec as P

MESH = pl.DeviceIdType.MESH
F32 = jnp.float32
epsilon_norm = 1e-05
discount = 1.0
trace_decay = 0.999
penalty_weight = 0.1

OFFSETS = (None, 1, -1, 2, -2, 3, -3, 4, 0)
SLOT = {0: 8, 1: 1, -1: 2, 2: 3, -2: 4, 3: 5, -3: 6, 4: 7, -4: 7}
ORDER = (0, 2, 1, 3)


def kernel(
    hidden_hbm, layer_hbm, gains_hbm, w_hbm, targets_hbm, values_hbm, rewards_hbm, ref_hbm, end_hbm,
    out_ref,
    hid, lay, gains, w_own, w_peer, tgt, val, rew, ref, end,
    tok, layc, inv, a12, b12, a56, b56, a7, b7, want, inf, s1, s2, lps,
    load_sem, known_sem, w_sem, z_sem, piece_sem, inf_sem, extra_sem, xy_sem, send_sem, small_recv, small_send,
):
    x, y, z, c = (lax.axis_index(a) for a in ("x", "y", "z", "core"))
    width = hid.shape[1]
    acc12, acc56, acc7 = (a12, b12), (a56, b56), (a7, b7)
    cols = w_own.shape[0]
    xp, xm = lax.rem(x + 1, 4), lax.rem(x + 3, 4)
    yp, ym = lax.rem(y + 1, 4), lax.rem(y + 3, 4)
    zp, zm = lax.rem(z + 1, 8), lax.rem(z + 7, 8)
    b = 2 * z + c
    v = 4 * y + x

    qa = lax.rem(x + 2 * y, 4)
    qb = lax.rem(2 * x + y, 4)
    step = width // 16

    def start_col(t, k=0):
        first = lax.rem(qa + k, 4) * 2 * step if t < 2 else width // 2 + lax.rem(qb + k, 4) * 2 * step
        return pl.multiple_of(first + (t % 2) * step, step)

    def hid_load(k):
        rows = pl.ds(32 * k, 32)
        return pltpu.make_async_copy(hidden_hbm.at[rows, :], hid.at[rows, :], load_sem.at[k])

    for k in range(4):
        hid_load(k).start()
    layer_load = pltpu.make_async_copy(layer_hbm, lay, load_sem.at[8])
    layer_load.start()
    gains_load = pltpu.make_async_copy(gains_hbm, gains, load_sem.at[9])
    gains_load.start()

    barrier = pltpu.get_barrier_semaphore()
    in_plane = [{"x": xp}, {"x": xm}, {"y": yp}, {"y": ym}]
    for where in ({"z": zp}, {"z": zm}, *in_plane, {"core": 1 - c}):
        pl.semaphore_signal(barrier, inc=1, device_id=where, device_id_type=MESH)

    def tell(k):
        for where in in_plane:
            pl.semaphore_signal(known_sem.at[k], inc=1, device_id=where, device_id_type=MESH)

    w_load = pltpu.make_async_copy(w_hbm, w_own, w_sem.at[0])
    w_load.start()
    small = ((targets_hbm, tgt), (values_hbm, val), (rewards_hbm, rew), (ref_hbm, ref), (end_hbm, end))
    loads = [pltpu.make_async_copy(a, o, load_sem.at[10 + i]) for i, (a, o) in enumerate(small)]
    for load in loads:
        load.start()

    row_i = lax.broadcasted_iota(jnp.int32, (128, 128), 0)
    lane_i = lax.broadcasted_iota(jnp.int32, (128, 128), 1)
    eye = row_i == lane_i

    def as_column(line):
        return jnp.sum(jnp.where(eye, jnp.broadcast_to(line, (128, 128)), 0.0), axis=1, keepdims=True)

    with jax.named_scope("loadw"):
        layer_load.wait()
        for k in range(4):
            hid_load(k).wait()
            for r in range(32 * k, 32 * k + 32, 16):
                states = hid[r : r + 16, :].astype(F32)
                mean = jnp.mean(states * states, axis=1, keepdims=True)
                inv[r : r + 16, :] = jnp.broadcast_to(lax.rsqrt(mean + epsilon_norm), (16, 128))
        gains_load.wait()
    layc[...] = jnp.broadcast_to(as_column(lay[...].astype(F32)), (128, 128))

    def normalize(col):
        for half in range(step // 128):
            at = pl.ds(pl.multiple_of(col + 128 * half, 128), 128)
            which = layc[...]
            scaling = jnp.broadcast_to(gains[0:1, at], (128, 128))
            for e in range(1, 8):
                scaling = jnp.where(which == float(e), gains[e : e + 1, at], scaling)
            tok[896:1024, at] = (hid[:, at].astype(F32) * inv[...] * scaling).astype(jnp.bfloat16)

    def tile(slot, t, piece=None, k=0):
        row = (slot - 1) * 128
        rows = pl.ds(row, 128) if piece is None else pl.ds(row + 32 * piece, 32)
        return tok.at[rows, pl.ds(start_col(t, k), step)]

    def send(src, dst, recv, where):
        pltpu.make_async_remote_copy(
            src_ref=src, dst_ref=dst, send_sem=send_sem.at[0], recv_sem=recv, device_id=where, device_id_type=MESH
        ).start()

    def arrived(slot, t, piece):
        return z_sem.at[slot, t] if piece is None else piece_sem.at[slot, 4 * t + piece]

    def send_z(src_slot, t, up, piece=None):
        dst_slot = SLOT[OFFSETS[src_slot] + (-1 if up else 1)]
        send(tile(src_slot, t, piece), tile(dst_slot, t, piece), arrived(dst_slot, t, piece), {"z": zp if up else zm})

    def send_xy(slot, t, piece=None):
        targets = [{"x": xp}, {"x": xm}] if t < 2 else [{"y": yp}, {"y": ym}]
        if slot > 2:
            targets.append((({"y": yp}, {"y": ym}) if t < 2 else ({"x": xp}, {"x": xm}))[t % 2])
        for where in targets:
            send(tile(slot, t, piece), tile(slot, t, piece), xy_sem.at[slot, t], where)

    def send_extra(half):
        for t in (half, half + 2):
            send(tile(8, t, k=2), tile(2, t, k=2), extra_sem.at[1, t], {"z": zp})
            send(tile(8, t, k=2), tile(1, t, k=2), extra_sem.at[0, t], {"z": zm})

    def wait_z(slot, t, piece=None):
        there = tile(slot, t, piece)
        pltpu.make_async_copy(there, there, arrived(slot, t, piece)).wait()

    FIRST = [(t, piece) for half in (0, 1) for piece in range(4) for t in (half, half + 2)]
    with jax.named_scope("norm2"):
        normalize(start_col(0))
        normalize(start_col(2))
    with jax.named_scope("barrier"):
        pl.semaphore_wait(barrier, 7)
    for t, piece in FIRST[:8]:
        send_z(8, t, True, piece)
        send_z(8, t, False, piece)
    normalize(start_col(1))
    normalize(start_col(3))
    for t, piece in FIRST[8:]:
        send_z(8, t, True, piece)
        send_z(8, t, False, piece)

    def swap(k):
        part = pl.ds(k * (width // 8), width // 8)
        pltpu.make_async_remote_copy(
            src_ref=w_hbm.at[:, part], dst_ref=w_peer.at[:, part], send_sem=w_sem.at[1], recv_sem=w_sem.at[2],
            device_id={"core": 1 - c}, device_id_type=MESH,
        ).start()

    swap(0)
    swap(1)
    for load in loads:
        load.wait()

    sub = lax.broadcasted_iota(jnp.int32, (8, 128), 0)
    lanes = lax.broadcasted_iota(jnp.int32, (8, 128), 1)

    def packed(first, second, third):
        return jnp.where(sub == 0, first, jnp.where(sub == 1, second, jnp.where(sub == 2, third, 0.0)))

    def inf_at(core, j):
        return pl.ds(pl.multiple_of(core * 64 + 8 * j, 8), 8)

    inf[inf_at(c, 0), :] = packed(
        val[...], rew[...] + penalty_weight * ref[...] - val[...], 1.0 - end[...].astype(F32)
    )
    def inf_tile(slot):
        return inf.at[inf_at(c, OFFSETS[slot] % 8), :]

    def send_inf(src_slot, up):
        slot = SLOT[OFFSETS[src_slot] + (-1 if up else 1)]
        pltpu.make_async_remote_copy(
            src_ref=inf_tile(src_slot), dst_ref=inf_tile(slot), send_sem=small_send.at[0], recv_sem=inf_sem.at[slot],
            device_id={"z": zp if up else zm}, device_id_type=MESH,
        ).start()

    def wait_inf(slot):
        pltpu.make_async_copy(inf_tile(slot), inf_tile(slot), inf_sem.at[slot]).wait()

    send_inf(8, True)
    send_inf(8, False)

    def rest(k, _):
        for t in range(4):
            normalize(start_col(t, k))
        return 0

    with jax.named_scope("rest"):
        lax.fori_loop(1, 4, rest, 0)

    for slot in range(1, 9):
        line = tgt[pl.ds(2 * lax.rem(z + OFFSETS[slot] + 8, 8) + c, 1), :]
        want[:, (slot - 1) * 128 : (slot - 1) * 128 + 128] = line

    own_start = (b * 16 + v) * cols
    peer_start = ((2 * z + 1 - c) * 16 + v) * cols
    contract = (((1,), (1,)), ((), ()))

    def score(slots, now=True):
        at = pl.ds((slots[0] - 1) * 128, 128 * len(slots))
        own = lax.dot_general(w_own[...], tok[at, :], contract, preferred_element_type=F32)
        peer = lax.dot_general(w_peer[...], tok[at, :], contract, preferred_element_type=F32)
        reduce(slots, own, peer, now)

    def mac(slots, sums, t, k, tiles=2, start=False):
        at = pl.ds((slots[0] - 1) * 128, 128 * len(slots))
        depth = pl.ds(start_col(t, k), tiles * step)
        for weights, total in zip((w_own, w_peer), sums):
            part = lax.dot_general(weights[:, depth], tok[at, depth], contract, preferred_element_type=F32)
            total[...] = part if start else total[...] + part

    def reduce(slots, own, peer, now=True):
        slot, count = slots[0], 128 * len(slots)
        top = jnp.maximum(jnp.max(own, axis=0, keepdims=True), jnp.max(peer, axis=0, keepdims=True))
        total = jnp.sum(jnp.exp(own - top), axis=0, keepdims=True) + jnp.sum(jnp.exp(peer - top), axis=0, keepdims=True)
        wanted = want[:, (slot - 1) * 128 : (slot - 1) * 128 + count]
        columns = lax.broadcasted_iota(jnp.int32, (cols, count), 0)
        pick = jnp.sum(jnp.where(columns == wanted - own_start, own, 0.0), axis=0, keepdims=True) + jnp.sum(
            jnp.where(columns == wanted - peer_start, peer, 0.0), axis=0, keepdims=True
        )
        for k, slot in enumerate(slots):
            cut = slice(128 * k, 128 * k + 128)
            j = OFFSETS[slot] % 8
            s1[0, 8 * j : 8 * j + 8, :] = packed(top[:, cut], total[:, cut], pick[:, cut])
        for slot in slots if now else ():
            send_part(slot)

    def send_part(slot):
            j = OFFSETS[slot] % 8
            for d in range(1, 8):
                pltpu.make_async_remote_copy(
                    src_ref=s1.at[0, pl.ds(8 * j, 8), :], dst_ref=s1.at[8 - d, pl.ds(8 * ((j - d) % 8), 8), :],
                    send_sem=small_send.at[1], recv_sem=small_recv.at[1],
                    device_id={"z": lax.rem(z + d, 8)}, device_id_type=MESH,
                ).start()

    def wait_xy(slot, t):
        tiles = tok.at[pl.ds(0, 128), pl.ds(0, step * (3 if slot > 2 else 2))]
        pltpu.make_async_copy(tiles, tiles, xy_sem.at[slot, t]).wait()

    def arrivals(phase, between=()):
        up_slot, down_slot = (SLOT[-phase], SLOT[phase])
        for n, (t, piece) in enumerate(FIRST if phase < 3 else [(t, None) for t in ORDER]):
            if phase < 4:
                onward = phase == 1 or piece in (None, 3)
                through = piece if phase == 1 else None
                wait_z(up_slot, t, piece)
                if onward and (phase < 3 or t % 2 == 0):
                    send_z(up_slot, t, True, through)
                send_xy(up_slot, t, piece)
                wait_z(down_slot, t, piece)
                if onward and (phase < 3 or t % 2 == 1):
                    send_z(down_slot, t, False, through)
                send_xy(down_slot, t, piece)
                for work in between[2 * n : 2 * n + 2]:
                    mac(*work)
                if phase == 1 and 4 <= n < 16 and n % 2 == 0:
                    swap(n // 2)
            else:
                wait_z(7, t)
                send_xy(7, t)

        if phase < 4:
            wait_inf(up_slot)
            send_inf(up_slot, True)
            wait_inf(down_slot)
            if phase < 3:
                send_inf(down_slot, False)
        else:
            wait_inf(7)

    def wait_extra(slot, t):
        there = tile(slot, t, k=2)
        pltpu.make_async_copy(there, there, extra_sem.at[slot - 1, t]).wait()

    tell(0)
    with jax.named_scope("arrive1"):
        arrivals(1)
    with jax.named_scope("arrive2"):
        arrivals(2)
    send_extra(0)
    pl.semaphore_wait(known_sem.at[0], 4)
    tell(1)
    with jax.named_scope("wload"):
        w_load.wait()
        pltpu.make_async_copy(w_peer, w_peer, w_sem.at[2]).wait()
    with jax.named_scope("score8"):
        score((8,), False)
    with jax.named_scope("waitxy12"):
        for t in range(4):
            wait_xy(1, t)
            wait_xy(2, t)
    with jax.named_scope("arrive3"):
        arrivals(3, [((1, 2), acc12, t, k, 2, t + k == 0) for k in (0, 1, 3) for t in (0, 2)])
    send_extra(1)
    with jax.named_scope("mac56n"):
        mac((5, 6), acc56, 0, 0, start=True)
        mac((5, 6), acc56, 2, 0)
    with jax.named_scope("waitxy34"):
        for t in range(4):
            wait_xy(3, t)
            wait_xy(4, t)
    with jax.named_scope("score34"):
        score((3, 4), False)

    def arrived_mac(slots, sums, t):
        with jax.named_scope(f"wait{slots[0]}{t}"):
            for slot in slots:
                wait_xy(slot, t)
        with jax.named_scope(f"mac{slots[0]}{t}"):
            for k in (1, 2, 3):
                mac(slots, sums, t, k, 1)

    def extra_mac(t):
        with jax.named_scope(f"waitex{t}"):
            wait_extra(1, t)
            wait_extra(2, t)
        mac((1, 2), acc12, t, 2, 1)

    arrived_mac((5, 6), acc56, 0)
    extra_mac(0)
    extra_mac(2)
    pl.semaphore_wait(known_sem.at[1], 4)
    tell(2)
    with jax.named_scope("arrive4"):
        arrivals(4)
    for slot in (8, 3, 4):
        send_part(slot)
    own_inf = inf.at[pl.ds(pl.multiple_of(64 * c, 8), 64), :]
    inf_send = pltpu.make_async_remote_copy(
        src_ref=own_inf, dst_ref=own_inf, send_sem=small_send.at[4], recv_sem=small_recv.at[4],
        device_id={"core": 1 - c}, device_id_type=MESH,
    )
    inf_send.start()
    with jax.named_scope("mac7n"):
        mac((7,), acc7, 0, 0, start=True)
        mac((7,), acc7, 2, 0)

    arrived_mac((5, 6), acc56, 2)
    with jax.named_scope("pre"):
        inf_send.wait()
        known = []
        vals = [inf[pl.ds(64 * core, 8, stride=8), :] for core in range(2)]
        after = [vals[1], jnp.where(sub + z == 7, 0.0, pltpu.roll(vals[0], 7, 0))]
        steps = (1, 2, 4, 8, 16, 32, 64)
        for core in range(2):
            base = inf[pl.ds(64 * core + 1, 8, stride=8), :]
            keeping = inf[pl.ds(64 * core + 2, 8, stride=8), :]
            following = jnp.where(lanes < 127, pltpu.roll(vals[core], 127, 1), pltpu.roll(after[core], 127, 1))
            factor = discount * trace_decay * keeping
            factors = []
            for k in steps:
                factors.append(factor)
                factor = factor * jnp.where(lanes < 128 - k, pltpu.roll(factor, 128 - k, 1), 1.0)
            known.append((base + discount * following * keeping, factors, factor))

    extra_mac(1)
    extra_mac(3)
    with jax.named_scope("reduce12"):
        reduce((1, 2), acc12[0][...], acc12[1][...])
    arrived_mac((5, 6), acc56, 1)
    arrived_mac((5, 6), acc56, 3)
    with jax.named_scope("reduce56"):
        reduce((5, 6), acc56[0][...], acc56[1][...])
    pl.semaphore_wait(known_sem.at[2], 4)
    arrived_mac((7,), acc7, 0)
    arrived_mac((7,), acc7, 2)
    arrived_mac((7,), acc7, 1)
    arrived_mac((7,), acc7, 3)
    with jax.named_scope("score7"):
        reduce((7,), acc7[0][...], acc7[1][...])

    with jax.named_scope("s1"):
        seven = s1.at[pl.ds(1, 7)]
        pltpu.make_async_copy(seven, seven, small_recv.at[1]).wait()

    def joined(tops):
        top = functools.reduce(jnp.maximum, tops)
        return top, [jnp.exp(t - top) for t in tops]

    top, shares = joined([s1[k, pl.ds(0, 8, stride=8), :] for k in range(8)])
    total = sum(s1[k, pl.ds(1, 8, stride=8), :] * shares[k] for k in range(8))
    s2[v, 0] = top + jnp.log(total)
    s2[v, 1] = sum(s1[k, pl.ds(2, 8, stride=8), :] for k in range(8))
    for k in range(1, 16):
        pltpu.make_async_remote_copy(
            src_ref=s2.at[v], dst_ref=s2.at[v], send_sem=small_send.at[2], recv_sem=small_recv.at[2],
            device_id={"y": lax.rem(y + k // 4, 4), "x": lax.rem(x + k % 4, 4)}, device_id_type=MESH,
        ).start()
    fifteen = s2.at[pl.ds(0, 15)]
    with jax.named_scope("s2"):
        pltpu.make_async_copy(fifteen, fifteen, small_recv.at[2]).wait()
    top, shares = joined([s2[k, 0] for k in range(16)])
    lps[c] = sum(s2[k, 1] for k in range(16)) - (top + jnp.log(sum(shares)))
    lp_send = pltpu.make_async_remote_copy(
        src_ref=lps.at[c], dst_ref=lps.at[c], send_sem=small_send.at[3], recv_sem=small_recv.at[3],
        device_id={"core": 1 - c}, device_id_type=MESH,
    )
    lp_send.start()
    with jax.named_scope("s3"):
        lp_send.wait()

    local = []
    for core in range(2):
        base, factors, _ = known[core]
        line = base - penalty_weight * lps[core]
        for k, f in zip(steps, factors):
            line = line + f * jnp.where(lanes < 128 - k, pltpu.roll(line, 128 - k, 1), 0.0)
        local.append(line)

    def spread(column):
        return jnp.broadcast_to(column, (8, 128))

    head = [spread(line[:, 0:1]) for line in local]
    prod = [spread(known[core][2][:, 0:1]) for core in range(2)]
    in_range = sub + z < 8
    tail = jnp.where(in_range, head[0] + prod[0] * head[1], 0.0)
    reach = jnp.where(in_range, prod[0] * prod[1], 0.0)
    for k in (1, 2, 4):
        tail = tail + reach * jnp.where(sub < 8 - k, pltpu.roll(tail, 8 - k, 0), 0.0)
        reach = reach * jnp.where(sub < 8 - k, pltpu.roll(reach, 8 - k, 0), 0.0)
    beyond = pltpu.roll(jnp.where(sub == 0, 0.0, tail), 7, 0)
    first = c == 0
    incoming = jnp.where(first, head[1] + prod[1] * beyond, beyond)
    mine = jnp.where(first, local[0], local[1]) + jnp.where(first, known[0][2], known[1][2]) * incoming
    out_ref[...] = jnp.where(sub == 0, lps[c], jnp.where(sub == 1, pltpu.roll(mine, 1, 0), 0.0))

    with jax.named_scope("endsend"):
        seven_blocks = tok.at[pl.ds(0, 896), :]
        pltpu.make_async_copy(seven_blocks, seven_blocks, send_sem.at[0]).wait()
        pltpu.make_async_copy(w_peer, w_peer, w_sem.at[1]).wait()
        others = inf.at[pl.ds(0, 56), :]
        pltpu.make_async_copy(others, others, small_send.at[0]).wait()
        pltpu.make_async_copy(seven, seven, small_send.at[1]).wait()
        pltpu.make_async_copy(fifteen, fifteen, small_send.at[2]).wait()


def per_device(hidden, exit_layer, exit_gains, unembed, targets, values, rewards, ref_logprob, segment_end):
    width, cols = unembed.shape
    line = lambda a: a.reshape(1, 128)
    anywhere = pl.BlockSpec(memory_space=pl.ANY)
    vmem = pl.BlockSpec(memory_space=pltpu.VMEM)
    i32 = jnp.int32
    both = pl.pallas_call(
        kernel,
        out_shape=jax.ShapeDtypeStruct((8, 128), F32),
        in_specs=[anywhere] * 9,
        out_specs=vmem,
        scratch_shapes=[
            pltpu.VMEM((128, width), jnp.bfloat16),
            pltpu.VMEM((1, 128), i32),
            pltpu.VMEM((8, width), F32),
            pltpu.VMEM((cols, width), jnp.bfloat16),
            pltpu.VMEM((cols, width), jnp.bfloat16),
            pltpu.VMEM((16, 128), i32),
            pltpu.VMEM((1, 128), F32),
            pltpu.VMEM((1, 128), F32),
            pltpu.VMEM((1, 128), F32),
            pltpu.VMEM((1, 128), i32),
            pltpu.VMEM((1024, width), jnp.bfloat16),
            pltpu.VMEM((128, 128), F32),
            pltpu.VMEM((128, 128), F32),
            pltpu.VMEM((cols, 256), F32),
            pltpu.VMEM((cols, 256), F32),
            pltpu.VMEM((cols, 256), F32),
            pltpu.VMEM((cols, 256), F32),
            pltpu.VMEM((cols, 128), F32),
            pltpu.VMEM((cols, 128), F32),
            pltpu.VMEM((1, 1024), i32),
            pltpu.VMEM((128, 128), F32),
            pltpu.VMEM((8, 64, 128), F32),
            pltpu.VMEM((16, 2, 8, 128), F32),
            pltpu.VMEM((2, 8, 128), F32),
            pltpu.SemaphoreType.DMA((15,)),
            pltpu.SemaphoreType.REGULAR((3,)),
            pltpu.SemaphoreType.DMA((3,)),
            pltpu.SemaphoreType.DMA((8, 4)),
            pltpu.SemaphoreType.DMA((5, 16)),
            pltpu.SemaphoreType.DMA((8,)),
            pltpu.SemaphoreType.DMA((2, 4)),
            pltpu.SemaphoreType.DMA((8, 4)),
            pltpu.SemaphoreType.DMA((1,)),
            pltpu.SemaphoreType.DMA((5,)),
            pltpu.SemaphoreType.DMA((5,)),
        ],
        compiler_params=pltpu.CompilerParams(
            collective_id=0, has_side_effects=True, vmem_limit_bytes=60 * 1024 * 1024
        ),
    )(
        hidden, line(exit_layer), exit_gains, unembed.T, targets.reshape(16, 128),
        line(values), line(rewards), line(ref_logprob), line(segment_end),
    )
    return both[0], both[1]


def solution(mesh):
    torus = Mesh(mesh.devices.reshape(8, 2, 4, 4), ("z", "core", "y", "x"))
    tokens = P(("z", "core"))
    return jax.shard_map(
        per_device,
        mesh=torus,
        in_specs=(
            P(("z", "core"), None), tokens, P(), P(None, ("z", "core", "y", "x")), P(), tokens, tokens, tokens, tokens,
        ),
        out_specs=(tokens, tokens),
        check_vma=False,
    )
```

```python
import functools

import jax
import jax.numpy as jnp
from jax import lax
from jax.experimental import pallas as pl
from jax.experimental.pallas import tpu as pltpu
from jax.sharding import Mesh
from jax.sharding import PartitionSpec as P

MESH = pl.DeviceIdType.MESH
F32 = jnp.float32
epsilon_norm = 1e-05
discount = 1.0
trace_decay = 0.999
penalty_weight = 0.1

OFFSETS = (None, 1, -1, 2, -2, 3, -3, 4, 0)
SLOT = {0: 8, 1: 1, -1: 2, 2: 3, -2: 4, 3: 5, -3: 6, 4: 7, -4: 7}
ORDER = (0, 2, 1, 3)


def kernel(
    hidden_hbm, layer_hbm, gains_hbm, w_hbm, targets_hbm, values_hbm, rewards_hbm, ref_hbm, end_hbm,
    out_ref,
    hid, lay, gains, w_own, w_peer, tgt, val, rew, ref, end,
    tok, layc, inv, a12, b12, a56, b56, a7, b7, want, inf, s1, s2, lps,
    load_sem, known_sem, w_sem, z_sem, piece_sem, inf_sem, s1_recv, extra_sem, xy_sem, send_sem, small_recv, small_send,
):
    x, y, z, c = (lax.axis_index(a) for a in ("x", "y", "z", "core"))
    width = hid.shape[1]
    acc12, acc56, acc7 = (a12, b12), (a56, b56), (a7, b7)
    cols = w_own.shape[0]
    xp, xm = lax.rem(x + 1, 4), lax.rem(x + 3, 4)
    yp, ym = lax.rem(y + 1, 4), lax.rem(y + 3, 4)
    zp, zm = lax.rem(z + 1, 8), lax.rem(z + 7, 8)
    b = 2 * z + c
    v = 4 * y + x

    qa = lax.rem(x + 2 * y, 4)
    qb = lax.rem(2 * x + y, 4)
    step = width // 16

    def start_col(t, k=0):
        first = lax.rem(qa + k, 4) * 2 * step if t < 2 else width // 2 + lax.rem(qb + k, 4) * 2 * step
        return pl.multiple_of(first + (t % 2) * step, step)

    def hid_load(k):
        rows = pl.ds(32 * k, 32)
        return pltpu.make_async_copy(hidden_hbm.at[rows, :], hid.at[rows, :], load_sem.at[k])

    for k in range(4):
        hid_load(k).start()
    layer_load = pltpu.make_async_copy(layer_hbm, lay, load_sem.at[8])
    layer_load.start()
    gains_load = pltpu.make_async_copy(gains_hbm, gains, load_sem.at[9])
    gains_load.start()

    barrier = pltpu.get_barrier_semaphore()
    in_plane = [{"x": xp}, {"x": xm}, {"y": yp}, {"y": ym}]
    for where in ({"z": zp}, {"z": zm}, *in_plane, {"core": 1 - c}):
        pl.semaphore_signal(barrier, inc=1, device_id=where, device_id_type=MESH)

    def tell(k):
        for where in in_plane:
            pl.semaphore_signal(known_sem.at[k], inc=1, device_id=where, device_id_type=MESH)

    w_load = pltpu.make_async_copy(w_hbm, w_own, w_sem.at[0])
    w_load.start()
    small = ((targets_hbm, tgt), (values_hbm, val), (rewards_hbm, rew), (ref_hbm, ref), (end_hbm, end))
    loads = [pltpu.make_async_copy(a, o, load_sem.at[10 + i]) for i, (a, o) in enumerate(small)]
    for load in loads:
        load.start()

    row_i = lax.broadcasted_iota(jnp.int32, (128, 128), 0)
    lane_i = lax.broadcasted_iota(jnp.int32, (128, 128), 1)
    eye = row_i == lane_i

    def as_column(line):
        return jnp.sum(jnp.where(eye, jnp.broadcast_to(line, (128, 128)), 0.0), axis=1, keepdims=True)

    with jax.named_scope("loadw"):
        layer_load.wait()
        for k in range(4):
            hid_load(k).wait()
            for r in range(32 * k, 32 * k + 32, 16):
                states = hid[r : r + 16, :].astype(F32)
                mean = jnp.mean(states * states, axis=1, keepdims=True)
                inv[r : r + 16, :] = jnp.broadcast_to(lax.rsqrt(mean + epsilon_norm), (16, 128))
        gains_load.wait()
    layc[...] = jnp.broadcast_to(as_column(lay[...].astype(F32)), (128, 128))

    def normalize(col):
        for half in range(step // 128):
            at = pl.ds(pl.multiple_of(col + 128 * half, 128), 128)
            which = layc[...]
            scaling = jnp.broadcast_to(gains[0:1, at], (128, 128))
            for e in range(1, 8):
                scaling = jnp.where(which == float(e), gains[e : e + 1, at], scaling)
            tok[896:1024, at] = (hid[:, at].astype(F32) * inv[...] * scaling).astype(jnp.bfloat16)

    def tile(slot, t, piece=None, k=0):
        row = (slot - 1) * 128
        rows = pl.ds(row, 128) if piece is None else pl.ds(row + 32 * piece, 32)
        return tok.at[rows, pl.ds(start_col(t, k), step)]

    def send(src, dst, recv, where):
        pltpu.make_async_remote_copy(
            src_ref=src, dst_ref=dst, send_sem=send_sem.at[0], recv_sem=recv, device_id=where, device_id_type=MESH
        ).start()

    def arrived(slot, t, piece):
        return z_sem.at[slot, t] if piece is None else piece_sem.at[slot, 4 * t + piece]

    def send_z(src_slot, t, up, piece=None):
        dst_slot = SLOT[OFFSETS[src_slot] + (-1 if up else 1)]
        send(tile(src_slot, t, piece), tile(dst_slot, t, piece), arrived(dst_slot, t, piece), {"z": zp if up else zm})

    def send_xy(slot, t, piece=None):
        targets = [{"x": xp}, {"x": xm}] if t < 2 else [{"y": yp}, {"y": ym}]
        if slot > 2:
            targets.append((({"y": yp}, {"y": ym}) if t < 2 else ({"x": xp}, {"x": xm}))[t % 2])
        for where in targets:
            send(tile(slot, t, piece), tile(slot, t, piece), xy_sem.at[slot, t], where)

    def send_extra(half):
        for t in (half, half + 2):
            send(tile(8, t, k=2), tile(2, t, k=2), extra_sem.at[1, t], {"z": zp})
            send(tile(8, t, k=2), tile(1, t, k=2), extra_sem.at[0, t], {"z": zm})

    def wait_z(slot, t, piece=None):
        there = tile(slot, t, piece)
        pltpu.make_async_copy(there, there, arrived(slot, t, piece)).wait()

    FIRST = [(t, piece) for half in (0, 1) for piece in range(4) for t in (half, half + 2)]
    with jax.named_scope("norm2"):
        normalize(start_col(0))
        normalize(start_col(2))
    with jax.named_scope("barrier"):
        pl.semaphore_wait(barrier, 7)
    for t, piece in FIRST[:8]:
        send_z(8, t, True, piece)
        send_z(8, t, False, piece)
    normalize(start_col(1))
    normalize(start_col(3))
    for t, piece in FIRST[8:]:
        send_z(8, t, True, piece)
        send_z(8, t, False, piece)

    def swap(k):
        part = pl.ds(k * (width // 8), width // 8)
        pltpu.make_async_remote_copy(
            src_ref=w_hbm.at[:, part], dst_ref=w_peer.at[:, part], send_sem=w_sem.at[1], recv_sem=w_sem.at[2],
            device_id={"core": 1 - c}, device_id_type=MESH,
        ).start()

    swap(0)
    swap(1)
    for load in loads:
        load.wait()

    sub = lax.broadcasted_iota(jnp.int32, (8, 128), 0)
    lanes = lax.broadcasted_iota(jnp.int32, (8, 128), 1)

    def packed(first, second, third):
        return jnp.where(sub == 0, first, jnp.where(sub == 1, second, jnp.where(sub == 2, third, 0.0)))

    def inf_at(core, j):
        return pl.ds(pl.multiple_of(core * 64 + 8 * j, 8), 8)

    inf[inf_at(c, 0), :] = packed(
        val[...], rew[...] + penalty_weight * ref[...] - val[...], 1.0 - end[...].astype(F32)
    )
    def inf_tile(slot):
        return inf.at[inf_at(c, OFFSETS[slot] % 8), :]

    def send_inf(src_slot, up):
        slot = SLOT[OFFSETS[src_slot] + (-1 if up else 1)]
        pltpu.make_async_remote_copy(
            src_ref=inf_tile(src_slot), dst_ref=inf_tile(slot), send_sem=small_send.at[0], recv_sem=inf_sem.at[slot],
            device_id={"z": zp if up else zm}, device_id_type=MESH,
        ).start()

    def wait_inf(slot):
        pltpu.make_async_copy(inf_tile(slot), inf_tile(slot), inf_sem.at[slot]).wait()

    send_inf(8, True)
    send_inf(8, False)

    def rest(k, _):
        for t in range(4):
            normalize(start_col(t, k))
        return 0

    with jax.named_scope("rest"):
        lax.fori_loop(1, 4, rest, 0)

    for slot in range(1, 9):
        line = tgt[pl.ds(2 * lax.rem(z + OFFSETS[slot] + 8, 8) + c, 1), :]
        want[:, (slot - 1) * 128 : (slot - 1) * 128 + 128] = line

    own_start = (b * 16 + v) * cols
    peer_start = ((2 * z + 1 - c) * 16 + v) * cols
    contract = (((1,), (1,)), ((), ()))

    def score(slots, now=True):
        at = pl.ds((slots[0] - 1) * 128, 128 * len(slots))
        own = lax.dot_general(w_own[...], tok[at, :], contract, preferred_element_type=F32)
        peer = lax.dot_general(w_peer[...], tok[at, :], contract, preferred_element_type=F32)
        reduce(slots, own, peer, now)

    def mac(slots, sums, t, k, tiles=2, start=False):
        at = pl.ds((slots[0] - 1) * 128, 128 * len(slots))
        depth = pl.ds(start_col(t, k), tiles * step)
        for weights, total in zip((w_own, w_peer), sums):
            part = lax.dot_general(weights[:, depth], tok[at, depth], contract, preferred_element_type=F32)
            total[...] = part if start else total[...] + part

    def reduce(slots, own, peer, now=True):
        slot, count = slots[0], 128 * len(slots)
        top = jnp.maximum(jnp.max(own, axis=0, keepdims=True), jnp.max(peer, axis=0, keepdims=True))
        total = jnp.sum(jnp.exp(own - top), axis=0, keepdims=True) + jnp.sum(jnp.exp(peer - top), axis=0, keepdims=True)
        wanted = want[:, (slot - 1) * 128 : (slot - 1) * 128 + count]
        columns = lax.broadcasted_iota(jnp.int32, (cols, count), 0)
        pick = jnp.sum(jnp.where(columns == wanted - own_start, own, 0.0), axis=0, keepdims=True) + jnp.sum(
            jnp.where(columns == wanted - peer_start, peer, 0.0), axis=0, keepdims=True
        )
        for k, slot in enumerate(slots):
            cut = slice(128 * k, 128 * k + 128)
            j = OFFSETS[slot] % 8
            s1[c, 0, 8 * j : 8 * j + 8, :] = packed(top[:, cut], total[:, cut], pick[:, cut])
        for slot in slots if now else ():
            send_part(slot)

    def part_copy(slot, d):
        j = OFFSETS[slot] % 8
        return pltpu.make_async_remote_copy(
            src_ref=s1.at[c, 0, pl.ds(8 * j, 8), :], dst_ref=s1.at[c, (8 - d) % 8, pl.ds(8 * ((j - d) % 8), 8), :],
            send_sem=small_send.at[1], recv_sem=s1_recv.at[c],
            device_id={"z": lax.rem(z + d, 8), "core": 1}, device_id_type=MESH,
        )

    def send_part(slot):
        for d in (4, 3, 5, 2, 6, 1, 7):
            part_copy(slot, d).start()

        @pl.when(c == 0)
        def _():
            part_copy(slot, 0).start()

    def wait_xy(slot, t):
        tiles = tok.at[pl.ds(0, 128), pl.ds(0, step * (3 if slot > 2 else 2))]
        pltpu.make_async_copy(tiles, tiles, xy_sem.at[slot, t]).wait()

    def arrivals(phase, between=()):
        up_slot, down_slot = (SLOT[-phase], SLOT[phase])
        for n, (t, piece) in enumerate(FIRST if phase < 3 else [(t, None) for t in ORDER]):
            if phase < 4:
                onward = phase == 1 or piece in (None, 3)
                through = piece if phase == 1 else None
                wait_z(up_slot, t, piece)
                if onward and (phase < 3 or t % 2 == 0):
                    send_z(up_slot, t, True, through)
                send_xy(up_slot, t, piece)
                wait_z(down_slot, t, piece)
                if onward and (phase < 3 or t % 2 == 1):
                    send_z(down_slot, t, False, through)
                send_xy(down_slot, t, piece)
                for work in between[2 * n : 2 * n + 2]:
                    mac(*work)
                if phase == 1 and 4 <= n < 16 and n % 2 == 0:
                    swap(n // 2)
            else:
                wait_z(7, t)
                send_xy(7, t)

        if phase < 4:
            wait_inf(up_slot)
            send_inf(up_slot, True)
            wait_inf(down_slot)
            if phase < 3:
                send_inf(down_slot, False)
        else:
            wait_inf(7)

    def wait_extra(slot, t):
        there = tile(slot, t, k=2)
        pltpu.make_async_copy(there, there, extra_sem.at[slot - 1, t]).wait()

    tell(0)
    with jax.named_scope("arrive1"):
        arrivals(1)
    with jax.named_scope("arrive2"):
        arrivals(2)
    send_extra(0)
    pl.semaphore_wait(known_sem.at[0], 4)
    tell(1)
    with jax.named_scope("wload"):
        w_load.wait()
        pltpu.make_async_copy(w_peer, w_peer, w_sem.at[2]).wait()
    with jax.named_scope("score8"):
        score((8,), False)
    with jax.named_scope("waitxy12"):
        for t in range(4):
            wait_xy(1, t)
            wait_xy(2, t)
    with jax.named_scope("arrive3"):
        arrivals(3, [((1, 2), acc12, t, k, 2, t + k == 0) for k in (0, 1, 3) for t in (0, 2)])
    send_extra(1)
    with jax.named_scope("mac56n"):
        mac((5, 6), acc56, 0, 0, start=True)
        mac((5, 6), acc56, 2, 0)
    with jax.named_scope("waitxy34"):
        for t in range(4):
            wait_xy(3, t)
            wait_xy(4, t)
    with jax.named_scope("score34"):
        score((3, 4), False)

    def arrived_mac(slots, sums, t):
        with jax.named_scope(f"wait{slots[0]}{t}"):
            for slot in slots:
                wait_xy(slot, t)
        with jax.named_scope(f"mac{slots[0]}{t}"):
            for k in (1, 2, 3):
                mac(slots, sums, t, k, 1)

    def extra_mac(t):
        with jax.named_scope(f"waitex{t}"):
            wait_extra(1, t)
            wait_extra(2, t)
        mac((1, 2), acc12, t, 2, 1)

    arrived_mac((5, 6), acc56, 0)
    extra_mac(0)
    extra_mac(2)
    pl.semaphore_wait(known_sem.at[1], 4)
    tell(2)
    with jax.named_scope("arrive4"):
        arrivals(4)
    for slot in (8, 3, 4):
        send_part(slot)
    own_inf = inf.at[pl.ds(pl.multiple_of(64 * c, 8), 64), :]
    inf_send = pltpu.make_async_remote_copy(
        src_ref=own_inf, dst_ref=own_inf, send_sem=small_send.at[4], recv_sem=small_recv.at[4],
        device_id={"core": 1 - c}, device_id_type=MESH,
    )
    inf_send.start()
    with jax.named_scope("mac7n"):
        mac((7,), acc7, 0, 0, start=True)
        mac((7,), acc7, 2, 0)

    arrived_mac((5, 6), acc56, 2)
    with jax.named_scope("pre"):
        inf_send.wait()
        known = []
        vals = [inf[pl.ds(64 * core, 8, stride=8), :] for core in range(2)]
        after = [vals[1], jnp.where(sub + z == 7, 0.0, pltpu.roll(vals[0], 7, 0))]
        steps = (1, 2, 4, 8, 16, 32, 64)
        for core in range(2):
            base = inf[pl.ds(64 * core + 1, 8, stride=8), :]
            keeping = inf[pl.ds(64 * core + 2, 8, stride=8), :]
            following = jnp.where(lanes < 127, pltpu.roll(vals[core], 127, 1), pltpu.roll(after[core], 127, 1))
            factor = discount * trace_decay * keeping
            factors = []
            for k in steps:
                factors.append(factor)
                factor = factor * jnp.where(lanes < 128 - k, pltpu.roll(factor, 128 - k, 1), 1.0)
            known.append((base + discount * following * keeping, factors, factor))

    extra_mac(1)
    extra_mac(3)
    with jax.named_scope("reduce12"):
        reduce((1, 2), acc12[0][...], acc12[1][...])
    arrived_mac((5, 6), acc56, 1)
    arrived_mac((5, 6), acc56, 3)
    with jax.named_scope("reduce56"):
        reduce((5, 6), acc56[0][...], acc56[1][...])
    pl.semaphore_wait(known_sem.at[2], 4)
    arrived_mac((7,), acc7, 0)
    arrived_mac((7,), acc7, 2)
    arrived_mac((7,), acc7, 1)
    arrived_mac((7,), acc7, 3)
    with jax.named_scope("score7"):
        reduce((7,), acc7[0][...], acc7[1][...])

    def joined(tops):
        top = functools.reduce(jnp.maximum, tops)
        return top, [jnp.exp(t - top) for t in tops]

    def lps_copy():
        return pltpu.make_async_remote_copy(
            src_ref=lps, dst_ref=lps, send_sem=small_send.at[3], recv_sem=small_recv.at[3],
            device_id={"core": 0}, device_id_type=MESH,
        )

    fifteen = s2.at[pl.ds(0, 15)]
    eight, seven = s1.at[0], s1.at[1, pl.ds(1, 7)]

    @pl.when(c == 1)
    def _():
        with jax.named_scope("s1"):
            pltpu.make_async_copy(seven, seven, s1_recv.at[1]).wait()
            pltpu.make_async_copy(eight, eight, s1_recv.at[0]).wait()
        for core in range(2):
            top, shares = joined([s1[core, k, pl.ds(0, 8, stride=8), :] for k in range(8)])
            total = sum(s1[core, k, pl.ds(1, 8, stride=8), :] * shares[k] for k in range(8))
            s2[v, 2 * core] = top + jnp.log(total)
            s2[v, 2 * core + 1] = sum(s1[core, k, pl.ds(2, 8, stride=8), :] for k in range(8))
        for k in (10, 6, 9, 11, 14, 2, 8, 5, 7, 13, 15, 1, 3, 4, 12):
            pltpu.make_async_remote_copy(
                src_ref=s2.at[v], dst_ref=s2.at[v], send_sem=small_send.at[2], recv_sem=small_recv.at[2],
                device_id={"y": lax.rem(y + k // 4, 4), "x": lax.rem(x + k % 4, 4)}, device_id_type=MESH,
            ).start()
        with jax.named_scope("s2"):
            pltpu.make_async_copy(fifteen, fifteen, small_recv.at[2]).wait()
        for core in range(2):
            top, shares = joined([s2[k, 2 * core] for k in range(16)])
            lps[core] = sum(s2[k, 2 * core + 1] for k in range(16)) - (top + jnp.log(sum(shares)))
        lps_copy().start()

    @pl.when(c == 0)
    def _():
        with jax.named_scope("s3"):
            lps_copy().wait_recv()

    local = []
    for core in range(2):
        base, factors, _ = known[core]
        line = base - penalty_weight * lps[core]
        for k, f in zip(steps, factors):
            line = line + f * jnp.where(lanes < 128 - k, pltpu.roll(line, 128 - k, 1), 0.0)
        local.append(line)

    def spread(column):
        return jnp.broadcast_to(column, (8, 128))

    head = [spread(line[:, 0:1]) for line in local]
    prod = [spread(known[core][2][:, 0:1]) for core in range(2)]
    in_range = sub + z < 8
    tail = jnp.where(in_range, head[0] + prod[0] * head[1], 0.0)
    reach = jnp.where(in_range, prod[0] * prod[1], 0.0)
    for k in (1, 2, 4):
        tail = tail + reach * jnp.where(sub < 8 - k, pltpu.roll(tail, 8 - k, 0), 0.0)
        reach = reach * jnp.where(sub < 8 - k, pltpu.roll(reach, 8 - k, 0), 0.0)
    beyond = pltpu.roll(jnp.where(sub == 0, 0.0, tail), 7, 0)
    first = c == 0
    incoming = jnp.where(first, head[1] + prod[1] * beyond, beyond)
    mine = jnp.where(first, local[0], local[1]) + jnp.where(first, known[0][2], known[1][2]) * incoming
    out_ref[...] = jnp.where(sub == 0, lps[c], jnp.where(sub == 1, pltpu.roll(mine, 1, 0), 0.0))

    with jax.named_scope("endsend"):
        seven_blocks = tok.at[pl.ds(0, 896), :]
        pltpu.make_async_copy(seven_blocks, seven_blocks, send_sem.at[0]).wait()
        pltpu.make_async_copy(w_peer, w_peer, w_sem.at[1]).wait()
        others = inf.at[pl.ds(0, 56), :]
        pltpu.make_async_copy(others, others, small_send.at[0]).wait()

        @pl.when(c == 0)
        def _():
            pltpu.make_async_copy(eight, eight, small_send.at[1]).wait()

        @pl.when(c == 1)
        def _():
            pltpu.make_async_copy(seven, seven, small_send.at[1]).wait()
            pltpu.make_async_copy(fifteen, fifteen, small_send.at[2]).wait()
            lps_copy().wait_send()


def per_device(hidden, exit_layer, exit_gains, unembed, targets, values, rewards, ref_logprob, segment_end):
    width, cols = unembed.shape
    line = lambda a: a.reshape(1, 128)
    anywhere = pl.BlockSpec(memory_space=pl.ANY)
    vmem = pl.BlockSpec(memory_space=pltpu.VMEM)
    i32 = jnp.int32
    both = pl.pallas_call(
        kernel,
        out_shape=jax.ShapeDtypeStruct((8, 128), F32),
        in_specs=[anywhere] * 9,
        out_specs=vmem,
        scratch_shapes=[
            pltpu.VMEM((128, width), jnp.bfloat16),
            pltpu.VMEM((1, 128), i32),
            pltpu.VMEM((8, width), F32),
            pltpu.VMEM((cols, width), jnp.bfloat16),
            pltpu.VMEM((cols, width), jnp.bfloat16),
            pltpu.VMEM((16, 128), i32),
            pltpu.VMEM((1, 128), F32),
            pltpu.VMEM((1, 128), F32),
            pltpu.VMEM((1, 128), F32),
            pltpu.VMEM((1, 128), i32),
            pltpu.VMEM((1024, width), jnp.bfloat16),
            pltpu.VMEM((128, 128), F32),
            pltpu.VMEM((128, 128), F32),
            pltpu.VMEM((cols, 256), F32),
            pltpu.VMEM((cols, 256), F32),
            pltpu.VMEM((cols, 256), F32),
            pltpu.VMEM((cols, 256), F32),
            pltpu.VMEM((cols, 128), F32),
            pltpu.VMEM((cols, 128), F32),
            pltpu.VMEM((1, 1024), i32),
            pltpu.VMEM((128, 128), F32),
            pltpu.VMEM((2, 8, 64, 128), F32),
            pltpu.VMEM((16, 4, 8, 128), F32),
            pltpu.VMEM((2, 8, 128), F32),
            pltpu.SemaphoreType.DMA((15,)),
            pltpu.SemaphoreType.REGULAR((3,)),
            pltpu.SemaphoreType.DMA((3,)),
            pltpu.SemaphoreType.DMA((8, 4)),
            pltpu.SemaphoreType.DMA((5, 16)),
            pltpu.SemaphoreType.DMA((8,)),
            pltpu.SemaphoreType.DMA((2,)),
            pltpu.SemaphoreType.DMA((2, 4)),
            pltpu.SemaphoreType.DMA((8, 4)),
            pltpu.SemaphoreType.DMA((1,)),
            pltpu.SemaphoreType.DMA((5,)),
            pltpu.SemaphoreType.DMA((5,)),
        ],
        compiler_params=pltpu.CompilerParams(
            collective_id=0, has_side_effects=True, vmem_limit_bytes=60 * 1024 * 1024
        ),
    )(
        hidden, line(exit_layer), exit_gains, unembed.T, targets.reshape(16, 128),
        line(values), line(rewards), line(ref_logprob), line(segment_end),
    )
    return both[0], both[1]


def solution(mesh):
    torus = Mesh(mesh.devices.reshape(8, 2, 4, 4), ("z", "core", "y", "x"))
    tokens = P(("z", "core"))
    return jax.shard_map(
        per_device,
        mesh=torus,
        in_specs=(
            P(("z", "core"), None), tokens, P(), P(None, ("z", "core", "y", "x")), P(), tokens, tokens, tokens, tokens,
        ),
        out_specs=(tokens, tokens),
        check_vma=False,
    )
```

```python
import functools

import jax
import jax.numpy as jnp
from jax import lax
from jax.experimental import pallas as pl
from jax.experimental.pallas import tpu as pltpu
from jax.sharding import Mesh
from jax.sharding import PartitionSpec as P

MESH = pl.DeviceIdType.MESH
F32 = jnp.float32
epsilon_norm = 1e-05
discount = 1.0
trace_decay = 0.999
penalty_weight = 0.1

OFFSETS = (None, 1, -1, 2, -2, 3, -3, 4, 0)
SLOT = {0: 8, 1: 1, -1: 2, 2: 3, -2: 4, 3: 5, -3: 6, 4: 7, -4: 7}
ORDER = (0, 2, 1, 3)


def kernel(
    hidden_hbm, layer_hbm, gains_hbm, w_hbm, targets_hbm, values_hbm, rewards_hbm, ref_hbm, end_hbm,
    out_ref,
    hid, lay, gains, w_own, w_peer, tgt, val, rew, ref, end,
    tok, layc, inv, a12, b12, a56, b56, a7, b7, want, inf, s1, s2, lps,
    load_sem, known_sem, w_sem, z_sem, piece_sem, inf_sem, s1_recv, extra_sem, xy_sem, send_sem, small_recv, small_send,
):
    x, y, z, c = (lax.axis_index(a) for a in ("x", "y", "z", "core"))
    width = hid.shape[1]
    acc12, acc56, acc7 = (a12, b12), (a56, b56), (a7, b7)
    cols = w_own.shape[0]
    xp, xm = lax.rem(x + 1, 4), lax.rem(x + 3, 4)
    yp, ym = lax.rem(y + 1, 4), lax.rem(y + 3, 4)
    zp, zm = lax.rem(z + 1, 8), lax.rem(z + 7, 8)
    b = 2 * z + c
    v = 4 * y + x

    qa = lax.rem(x + 2 * y, 4)
    qb = lax.rem(2 * x + y, 4)
    step = width // 16

    def start_col(t, k=0):
        first = lax.rem(qa + k, 4) * 2 * step if t < 2 else width // 2 + lax.rem(qb + k, 4) * 2 * step
        return pl.multiple_of(first + (t % 2) * step, step)

    def hid_load(k):
        rows = pl.ds(32 * k, 32)
        return pltpu.make_async_copy(hidden_hbm.at[rows, :], hid.at[rows, :], load_sem.at[k])

    for k in range(4):
        hid_load(k).start()
    layer_load = pltpu.make_async_copy(layer_hbm, lay, load_sem.at[8])
    layer_load.start()
    gains_load = pltpu.make_async_copy(gains_hbm, gains, load_sem.at[9])
    gains_load.start()

    barrier = pltpu.get_barrier_semaphore()
    in_plane = [{"x": xp}, {"x": xm}, {"y": yp}, {"y": ym}]
    for where in ({"z": zp}, {"z": zm}, *in_plane, {"core": 1 - c}):
        pl.semaphore_signal(barrier, inc=1, device_id=where, device_id_type=MESH)

    def tell(k):
        for where in in_plane:
            pl.semaphore_signal(known_sem.at[k], inc=1, device_id=where, device_id_type=MESH)

    w_load = pltpu.make_async_copy(w_hbm, w_own, w_sem.at[0])
    w_load.start()
    small = ((targets_hbm, tgt), (values_hbm, val), (rewards_hbm, rew), (ref_hbm, ref), (end_hbm, end))
    loads = [pltpu.make_async_copy(a, o, load_sem.at[10 + i]) for i, (a, o) in enumerate(small)]
    for load in loads:
        load.start()

    row_i = lax.broadcasted_iota(jnp.int32, (128, 128), 0)
    lane_i = lax.broadcasted_iota(jnp.int32, (128, 128), 1)
    eye = row_i == lane_i

    def as_column(line):
        return jnp.sum(jnp.where(eye, jnp.broadcast_to(line, (128, 128)), 0.0), axis=1, keepdims=True)

    with jax.named_scope("loadw"):
        layer_load.wait()
        for k in range(4):
            hid_load(k).wait()
            for r in range(32 * k, 32 * k + 32, 16):
                states = hid[r : r + 16, :].astype(F32)
                mean = jnp.mean(states * states, axis=1, keepdims=True)
                inv[r : r + 16, :] = jnp.broadcast_to(lax.rsqrt(mean + epsilon_norm), (16, 128))
        gains_load.wait()
    layc[...] = jnp.broadcast_to(as_column(lay[...].astype(F32)), (128, 128))

    def normalize(col):
        for half in range(step // 128):
            at = pl.ds(pl.multiple_of(col + 128 * half, 128), 128)
            which = layc[...]
            scaling = jnp.broadcast_to(gains[0:1, at], (128, 128))
            for e in range(1, 8):
                scaling = jnp.where(which == float(e), gains[e : e + 1, at], scaling)
            tok[896:1024, at] = (hid[:, at].astype(F32) * inv[...] * scaling).astype(jnp.bfloat16)

    def tile(slot, t, piece=None, k=0):
        row = (slot - 1) * 128
        rows = pl.ds(row, 128) if piece is None else pl.ds(row + 32 * piece, 32)
        return tok.at[rows, pl.ds(start_col(t, k), step)]

    def send(src, dst, recv, where):
        pltpu.make_async_remote_copy(
            src_ref=src, dst_ref=dst, send_sem=send_sem.at[0], recv_sem=recv, device_id=where, device_id_type=MESH
        ).start()

    def arrived(slot, t, piece):
        return z_sem.at[slot, t] if piece is None else piece_sem.at[slot, 4 * t + piece]

    def send_z(src_slot, t, up, piece=None):
        dst_slot = SLOT[OFFSETS[src_slot] + (-1 if up else 1)]
        send(tile(src_slot, t, piece), tile(dst_slot, t, piece), arrived(dst_slot, t, piece), {"z": zp if up else zm})

    def send_xy(slot, t, piece=None):
        targets = [{"x": xp}, {"x": xm}] if t < 2 else [{"y": yp}, {"y": ym}]
        if slot > 2:
            targets.append((({"y": yp}, {"y": ym}) if t < 2 else ({"x": xp}, {"x": xm}))[t % 2])
        for where in targets:
            send(tile(slot, t, piece), tile(slot, t, piece), xy_sem.at[slot, t], where)

    def send_extra(half):
        for t in (half, half + 2):
            send(tile(8, t, k=2), tile(2, t, k=2), extra_sem.at[1, t], {"z": zp})
            send(tile(8, t, k=2), tile(1, t, k=2), extra_sem.at[0, t], {"z": zm})

    def wait_z(slot, t, piece=None):
        there = tile(slot, t, piece)
        pltpu.make_async_copy(there, there, arrived(slot, t, piece)).wait()

    FIRST = [(t, piece) for half in (0, 1) for piece in range(4) for t in (half, half + 2)]
    with jax.named_scope("norm2"):
        normalize(start_col(0))
        normalize(start_col(2))
    with jax.named_scope("barrier"):
        pl.semaphore_wait(barrier, 7)
    for t, piece in FIRST[:8]:
        send_z(8, t, True, piece)
        send_z(8, t, False, piece)
    normalize(start_col(1))
    normalize(start_col(3))
    for t, piece in FIRST[8:]:
        send_z(8, t, True, piece)
        send_z(8, t, False, piece)

    def swap(k):
        part = pl.ds(k * (width // 8), width // 8)
        pltpu.make_async_remote_copy(
            src_ref=w_hbm.at[:, part], dst_ref=w_peer.at[:, part], send_sem=w_sem.at[1], recv_sem=w_sem.at[2],
            device_id={"core": 1 - c}, device_id_type=MESH,
        ).start()

    swap(0)
    swap(1)
    for load in loads:
        load.wait()

    sub = lax.broadcasted_iota(jnp.int32, (8, 128), 0)
    lanes = lax.broadcasted_iota(jnp.int32, (8, 128), 1)

    def packed(first, second, third):
        return jnp.where(sub == 0, first, jnp.where(sub == 1, second, jnp.where(sub == 2, third, 0.0)))

    def inf_at(core, j):
        return pl.ds(pl.multiple_of(core * 64 + 8 * j, 8), 8)

    inf[inf_at(c, 0), :] = packed(
        val[...], rew[...] + penalty_weight * ref[...] - val[...], 1.0 - end[...].astype(F32)
    )
    def inf_tile(slot):
        return inf.at[inf_at(c, OFFSETS[slot] % 8), :]

    def send_inf(src_slot, up):
        slot = SLOT[OFFSETS[src_slot] + (-1 if up else 1)]
        pltpu.make_async_remote_copy(
            src_ref=inf_tile(src_slot), dst_ref=inf_tile(slot), send_sem=small_send.at[0], recv_sem=inf_sem.at[slot],
            device_id={"z": zp if up else zm}, device_id_type=MESH,
        ).start()

    def wait_inf(slot):
        pltpu.make_async_copy(inf_tile(slot), inf_tile(slot), inf_sem.at[slot]).wait()

    send_inf(8, True)
    send_inf(8, False)

    def rest(k, _):
        for t in range(4):
            normalize(start_col(t, k))
        return 0

    with jax.named_scope("rest"):
        lax.fori_loop(1, 4, rest, 0)

    for slot in range(1, 9):
        line = tgt[pl.ds(2 * lax.rem(z + OFFSETS[slot] + 8, 8) + c, 1), :]
        want[:, (slot - 1) * 128 : (slot - 1) * 128 + 128] = line

    own_start = (b * 16 + v) * cols
    peer_start = ((2 * z + 1 - c) * 16 + v) * cols
    contract = (((1,), (1,)), ((), ()))

    def score(slots, now=True):
        at = pl.ds((slots[0] - 1) * 128, 128 * len(slots))
        own = lax.dot_general(w_own[...], tok[at, :], contract, preferred_element_type=F32)
        peer = lax.dot_general(w_peer[...], tok[at, :], contract, preferred_element_type=F32)
        reduce(slots, own, peer, now)

    def mac(slots, sums, t, k, tiles=2, start=False):
        at = pl.ds((slots[0] - 1) * 128, 128 * len(slots))
        depth = pl.ds(start_col(t, k), tiles * step)
        for weights, total in zip((w_own, w_peer), sums):
            part = lax.dot_general(weights[:, depth], tok[at, depth], contract, preferred_element_type=F32)
            total[...] = part if start else total[...] + part

    def reduce(slots, own, peer, now=True):
        slot, count = slots[0], 128 * len(slots)
        top = jnp.maximum(jnp.max(own, axis=0, keepdims=True), jnp.max(peer, axis=0, keepdims=True))
        total = jnp.sum(jnp.exp(own - top), axis=0, keepdims=True) + jnp.sum(jnp.exp(peer - top), axis=0, keepdims=True)
        wanted = want[:, (slot - 1) * 128 : (slot - 1) * 128 + count]
        columns = lax.broadcasted_iota(jnp.int32, (cols, count), 0)
        pick = jnp.sum(jnp.where(columns == wanted - own_start, own, 0.0), axis=0, keepdims=True) + jnp.sum(
            jnp.where(columns == wanted - peer_start, peer, 0.0), axis=0, keepdims=True
        )
        for k, slot in enumerate(slots):
            cut = slice(128 * k, 128 * k + 128)
            j = OFFSETS[slot] % 8
            s1[c, 0, 8 * j : 8 * j + 8, :] = packed(top[:, cut], total[:, cut], pick[:, cut])
        for slot in slots if now else ():
            send_part(slot)

    def part_copy(slot, d):
        j = OFFSETS[slot] % 8
        return pltpu.make_async_remote_copy(
            src_ref=s1.at[c, 0, pl.ds(8 * j, 8), :], dst_ref=s1.at[c, (8 - d) % 8, pl.ds(8 * ((j - d) % 8), 8), :],
            send_sem=small_send.at[1], recv_sem=s1_recv.at[c],
            device_id={"z": lax.rem(z + d, 8), "core": 1}, device_id_type=MESH,
        )

    def send_part(slot):
        for d in (4, 3, 5, 2, 6, 1, 7):
            part_copy(slot, d).start()

        @pl.when(c == 0)
        def _():
            part_copy(slot, 0).start()

    def wait_xy(slot, t):
        tiles = tok.at[pl.ds(0, 128), pl.ds(0, step * (3 if slot > 2 else 2))]
        pltpu.make_async_copy(tiles, tiles, xy_sem.at[slot, t]).wait()

    def arrivals(phase, between=()):
        up_slot, down_slot = (SLOT[-phase], SLOT[phase])
        for n, (t, piece) in enumerate(FIRST if phase < 3 else [(t, None) for t in ORDER]):
            if phase < 4:
                onward = phase == 1 or piece in (None, 3)
                through = piece if phase == 1 else None
                wait_z(up_slot, t, piece)
                if onward and (phase < 3 or t % 2 == 0):
                    send_z(up_slot, t, True, through)
                send_xy(up_slot, t, piece)
                wait_z(down_slot, t, piece)
                if onward and (phase < 3 or t % 2 == 1):
                    send_z(down_slot, t, False, through)
                send_xy(down_slot, t, piece)
                for work in between[2 * n : 2 * n + 2]:
                    mac(*work)
                if phase == 1 and 4 <= n < 16 and n % 2 == 0:
                    swap(n // 2)
            else:
                wait_z(7, t)
                send_xy(7, t)

        if phase < 4:
            wait_inf(up_slot)
            send_inf(up_slot, True)
            wait_inf(down_slot)
            if phase < 3:
                send_inf(down_slot, False)
        else:
            wait_inf(7)

    def wait_extra(slot, t):
        there = tile(slot, t, k=2)
        pltpu.make_async_copy(there, there, extra_sem.at[slot - 1, t]).wait()

    tell(0)
    with jax.named_scope("arrive1"):
        arrivals(1)
    with jax.named_scope("arrive2"):
        arrivals(2)
    send_extra(0)
    pl.semaphore_wait(known_sem.at[0], 4)
    tell(1)
    with jax.named_scope("wload"):
        w_load.wait()
        pltpu.make_async_copy(w_peer, w_peer, w_sem.at[2]).wait()
    with jax.named_scope("score8"):
        score((8,), False)
    with jax.named_scope("waitxy12"):
        for t in range(4):
            wait_xy(1, t)
            wait_xy(2, t)
    with jax.named_scope("arrive3"):
        arrivals(3, [((1, 2), acc12, t, k, 2, t + k == 0) for k in (0, 1, 3) for t in (0, 2)])
    send_extra(1)
    with jax.named_scope("mac56n"):
        mac((5, 6), acc56, 0, 0, start=True)
        mac((5, 6), acc56, 2, 0)
    with jax.named_scope("waitxy34"):
        for t in range(4):
            wait_xy(3, t)
            wait_xy(4, t)
    with jax.named_scope("score34"):
        score((3, 4), False)

    def arrived_mac(slots, sums, t):
        with jax.named_scope(f"wait{slots[0]}{t}"):
            for slot in slots:
                wait_xy(slot, t)
        with jax.named_scope(f"mac{slots[0]}{t}"):
            for k in (1, 2, 3):
                mac(slots, sums, t, k, 1)

    def extra_mac(t):
        with jax.named_scope(f"waitex{t}"):
            wait_extra(1, t)
            wait_extra(2, t)
        mac((1, 2), acc12, t, 2, 1)

    arrived_mac((5, 6), acc56, 0)
    extra_mac(0)
    extra_mac(2)
    pl.semaphore_wait(known_sem.at[1], 4)
    tell(2)
    with jax.named_scope("arrive4"):
        arrivals(4)
    for slot in (8, 3, 4):
        send_part(slot)
    own_inf = inf.at[pl.ds(pl.multiple_of(64 * c, 8), 64), :]
    inf_send = pltpu.make_async_remote_copy(
        src_ref=own_inf, dst_ref=own_inf, send_sem=small_send.at[4], recv_sem=small_recv.at[4],
        device_id={"core": 1 - c}, device_id_type=MESH,
    )
    inf_send.start()
    with jax.named_scope("mac7n"):
        mac((7,), acc7, 0, 0, start=True)
        mac((7,), acc7, 2, 0)

    arrived_mac((5, 6), acc56, 2)
    arrived_mac((5, 6), acc56, 1)
    arrived_mac((5, 6), acc56, 3)
    with jax.named_scope("reduce56"):
        reduce((5, 6), acc56[0][...], acc56[1][...])
    extra_mac(1)
    extra_mac(3)
    with jax.named_scope("reduce12"):
        reduce((1, 2), acc12[0][...], acc12[1][...])
    pl.semaphore_wait(known_sem.at[2], 4)
    arrived_mac((7,), acc7, 0)
    arrived_mac((7,), acc7, 2)
    arrived_mac((7,), acc7, 1)
    arrived_mac((7,), acc7, 3)
    with jax.named_scope("score7"):
        reduce((7,), acc7[0][...], acc7[1][...])

    with jax.named_scope("pre"):
        inf_send.wait()
        known = []
        vals = [inf[pl.ds(64 * core, 8, stride=8), :] for core in range(2)]
        after = [vals[1], jnp.where(sub + z == 7, 0.0, pltpu.roll(vals[0], 7, 0))]
        steps = (1, 2, 4, 8, 16, 32, 64)
        for core in range(2):
            base = inf[pl.ds(64 * core + 1, 8, stride=8), :]
            keeping = inf[pl.ds(64 * core + 2, 8, stride=8), :]
            following = jnp.where(lanes < 127, pltpu.roll(vals[core], 127, 1), pltpu.roll(after[core], 127, 1))
            factor = discount * trace_decay * keeping
            factors = []
            for k in steps:
                factors.append(factor)
                factor = factor * jnp.where(lanes < 128 - k, pltpu.roll(factor, 128 - k, 1), 1.0)
            known.append((base + discount * following * keeping, factors, factor))


    def joined(tops):
        top = functools.reduce(jnp.maximum, tops)
        return top, [jnp.exp(t - top) for t in tops]

    def lps_copy():
        return pltpu.make_async_remote_copy(
            src_ref=lps, dst_ref=lps, send_sem=small_send.at[3], recv_sem=small_recv.at[3],
            device_id={"core": 0}, device_id_type=MESH,
        )

    fifteen = s2.at[pl.ds(0, 15)]
    eight, seven = s1.at[0], s1.at[1, pl.ds(1, 7)]

    @pl.when(c == 1)
    def _():
        with jax.named_scope("s1"):
            pltpu.make_async_copy(seven, seven, s1_recv.at[1]).wait()
            pltpu.make_async_copy(eight, eight, s1_recv.at[0]).wait()
        for core in range(2):
            top, shares = joined([s1[core, k, pl.ds(0, 8, stride=8), :] for k in range(8)])
            total = sum(s1[core, k, pl.ds(1, 8, stride=8), :] * shares[k] for k in range(8))
            s2[v, 2 * core] = top + jnp.log(total)
            s2[v, 2 * core + 1] = sum(s1[core, k, pl.ds(2, 8, stride=8), :] for k in range(8))
        for k in (10, 6, 9, 11, 14, 2, 8, 5, 7, 13, 15, 1, 3, 4, 12):
            pltpu.make_async_remote_copy(
                src_ref=s2.at[v], dst_ref=s2.at[v], send_sem=small_send.at[2], recv_sem=small_recv.at[2],
                device_id={"y": lax.rem(y + k // 4, 4), "x": lax.rem(x + k % 4, 4)}, device_id_type=MESH,
            ).start()
        with jax.named_scope("s2"):
            pltpu.make_async_copy(fifteen, fifteen, small_recv.at[2]).wait()
        for core in range(2):
            top, shares = joined([s2[k, 2 * core] for k in range(16)])
            lps[core] = sum(s2[k, 2 * core + 1] for k in range(16)) - (top + jnp.log(sum(shares)))
        lps_copy().start()

    @pl.when(c == 0)
    def _():
        with jax.named_scope("s3"):
            lps_copy().wait_recv()

    local = []
    for core in range(2):
        base, factors, _ = known[core]
        line = base - penalty_weight * lps[core]
        for k, f in zip(steps, factors):
            line = line + f * jnp.where(lanes < 128 - k, pltpu.roll(line, 128 - k, 1), 0.0)
        local.append(line)

    def spread(column):
        return jnp.broadcast_to(column, (8, 128))

    head = [spread(line[:, 0:1]) for line in local]
    prod = [spread(known[core][2][:, 0:1]) for core in range(2)]
    in_range = sub + z < 8
    tail = jnp.where(in_range, head[0] + prod[0] * head[1], 0.0)
    reach = jnp.where(in_range, prod[0] * prod[1], 0.0)
    for k in (1, 2, 4):
        tail = tail + reach * jnp.where(sub < 8 - k, pltpu.roll(tail, 8 - k, 0), 0.0)
        reach = reach * jnp.where(sub < 8 - k, pltpu.roll(reach, 8 - k, 0), 0.0)
    beyond = pltpu.roll(jnp.where(sub == 0, 0.0, tail), 7, 0)
    first = c == 0
    incoming = jnp.where(first, head[1] + prod[1] * beyond, beyond)
    mine = jnp.where(first, local[0], local[1]) + jnp.where(first, known[0][2], known[1][2]) * incoming
    out_ref[...] = jnp.where(sub == 0, lps[c], jnp.where(sub == 1, pltpu.roll(mine, 1, 0), 0.0))

    with jax.named_scope("endsend"):
        seven_blocks = tok.at[pl.ds(0, 896), :]
        pltpu.make_async_copy(seven_blocks, seven_blocks, send_sem.at[0]).wait()
        pltpu.make_async_copy(w_peer, w_peer, w_sem.at[1]).wait()
        others = inf.at[pl.ds(0, 56), :]
        pltpu.make_async_copy(others, others, small_send.at[0]).wait()

        @pl.when(c == 0)
        def _():
            pltpu.make_async_copy(eight, eight, small_send.at[1]).wait()

        @pl.when(c == 1)
        def _():
            pltpu.make_async_copy(seven, seven, small_send.at[1]).wait()
            pltpu.make_async_copy(fifteen, fifteen, small_send.at[2]).wait()
            lps_copy().wait_send()


def per_device(hidden, exit_layer, exit_gains, unembed, targets, values, rewards, ref_logprob, segment_end):
    width, cols = unembed.shape
    line = lambda a: a.reshape(1, 128)
    anywhere = pl.BlockSpec(memory_space=pl.ANY)
    vmem = pl.BlockSpec(memory_space=pltpu.VMEM)
    i32 = jnp.int32
    both = pl.pallas_call(
        kernel,
        out_shape=jax.ShapeDtypeStruct((8, 128), F32),
        in_specs=[anywhere] * 9,
        out_specs=vmem,
        scratch_shapes=[
            pltpu.VMEM((128, width), jnp.bfloat16),
            pltpu.VMEM((1, 128), i32),
            pltpu.VMEM((8, width), F32),
            pltpu.VMEM((cols, width), jnp.bfloat16),
            pltpu.VMEM((cols, width), jnp.bfloat16),
            pltpu.VMEM((16, 128), i32),
            pltpu.VMEM((1, 128), F32),
            pltpu.VMEM((1, 128), F32),
            pltpu.VMEM((1, 128), F32),
            pltpu.VMEM((1, 128), i32),
            pltpu.VMEM((1024, width), jnp.bfloat16),
            pltpu.VMEM((128, 128), F32),
            pltpu.VMEM((128, 128), F32),
            pltpu.VMEM((cols, 256), F32),
            pltpu.VMEM((cols, 256), F32),
            pltpu.VMEM((cols, 256), F32),
            pltpu.VMEM((cols, 256), F32),
            pltpu.VMEM((cols, 128), F32),
            pltpu.VMEM((cols, 128), F32),
            pltpu.VMEM((1, 1024), i32),
            pltpu.VMEM((128, 128), F32),
            pltpu.VMEM((2, 8, 64, 128), F32),
            pltpu.VMEM((16, 4, 8, 128), F32),
            pltpu.VMEM((2, 8, 128), F32),
            pltpu.SemaphoreType.DMA((15,)),
            pltpu.SemaphoreType.REGULAR((3,)),
            pltpu.SemaphoreType.DMA((3,)),
            pltpu.SemaphoreType.DMA((8, 4)),
            pltpu.SemaphoreType.DMA((5, 16)),
            pltpu.SemaphoreType.DMA((8,)),
            pltpu.SemaphoreType.DMA((2,)),
            pltpu.SemaphoreType.DMA((2, 4)),
            pltpu.SemaphoreType.DMA((8, 4)),
            pltpu.SemaphoreType.DMA((1,)),
            pltpu.SemaphoreType.DMA((5,)),
            pltpu.SemaphoreType.DMA((5,)),
        ],
        compiler_params=pltpu.CompilerParams(
            collective_id=0, has_side_effects=True, vmem_limit_bytes=60 * 1024 * 1024
        ),
    )(
        hidden, line(exit_layer), exit_gains, unembed.T, targets.reshape(16, 128),
        line(values), line(rewards), line(ref_logprob), line(segment_end),
    )
    return both[0], both[1]


def solution(mesh):
    torus = Mesh(mesh.devices.reshape(8, 2, 4, 4), ("z", "core", "y", "x"))
    tokens = P(("z", "core"))
    return jax.shard_map(
        per_device,
        mesh=torus,
        in_specs=(
            P(("z", "core"), None), tokens, P(), P(None, ("z", "core", "y", "x")), P(), tokens, tokens, tokens, tokens,
        ),
        out_specs=(tokens, tokens),
        check_vma=False,
    )
```
